32 devices in a mesh: rep: 1 (over z), dp: 32 (over x, y, core).
Axes of the slice: x: 4, y: 4, z: 1, core: 2. Of those that a mesh axis runs over, the one named last changes fastest.
The devices are a block of a 4x4x8 slice.
Arguments:
- x: bfloat16 [32, 2048, 1280], P(('rep', 'dp'))
- dy: bfloat16 [32, 2048, 1280], P(('rep', 'dp'))
- w_gate: bfloat16 [2, 1280, 4480], replicated
- w_up: bfloat16 [2, 1280, 4480], replicated
- w_down: bfloat16 [2, 4480, 1280], replicated
- m_w_gate: float32 [2, 1280, 4480], P(None, 'dp')
- m_w_up: float32 [2, 1280, 4480], P(None, 'dp')
- m_w_down: float32 [2, 4480, 1280], P(None, 'dp')
- v_w_gate: float32 [2, 1280, 4480], P(None, 'dp')
- v_w_up: float32 [2, 1280, 4480], P(None, 'dp')
- v_w_down: float32 [2, 4480, 1280], P(None, 'dp')
Outputs:
- output 1: bfloat16 [2, 1280, 4480], P('rep')
- output 2: bfloat16 [2, 1280, 4480], P('rep')
- output 3: bfloat16 [2, 4480, 1280], P('rep')
- output 4: float32 [2, 1280, 4480], P('rep', 'dp')
- output 5: float32 [2, 1280, 4480], P('rep', 'dp')
- output 6: float32 [2, 4480, 1280], P('rep', 'dp')
- output 7: float32 [2, 1280, 4480], P('rep', 'dp')
- output 8: float32 [2, 1280, 4480], P('rep', 'dp')
- output 9: float32 [2, 4480, 1280], P('rep', 'dp')
All inputs are finite; a program needn't handle non-finite values.
Results may differ from the reference program's by a relative error of at most 0.022.
Values are sent between devices in bfloat16 or wider.
A program may use at most 768 MiB of HBM per device.

```python
import jax
import jax.numpy as jnp
from jax import lax

SEQUENCES = 32
TOKENS = 2048
D = 1280
FF = 4480
LAYERS = 2
NAMES = ("w_gate", "w_up", "w_down")
SHAPES = {"w_gate": (LAYERS, D, FF), "w_up": (LAYERS, D, FF), "w_down": (LAYERS, FF, D)}


def bump(key, n, height):
    away = (jnp.arange(n, dtype=jnp.int32) - jax.random.randint(key, (), 0, n, jnp.int32)) % n
    return jnp.where(away < n // 8, height, 1.0)


def together(key, own, strength):
    shared = jax.random.normal(key, own.shape[1:], jnp.float32)
    return (own + strength * shared) * lax.rsqrt(1 + strength * strength)


def setup_inputs(seed: int = 0, part: int = 0) -> dict:
    kx, kdy, ka, kb, kz, kf, kh, kl, *keys = jax.random.split(jax.random.key(seed), 8 + 3 * len(NAMES))
    kx, kdy, ka, kb = (jax.random.fold_in(k, part) for k in (kx, kdy, ka, kb))
    kw, km, kv = (keys[i::3] for i in range(3))
    shape = (SEQUENCES, TOKENS, D)
    much_x, much_dy = jax.random.uniform(kz, (2,), jnp.float32, 0.0, 1.0)
    loud = 2.0 ** jax.random.uniform(jax.random.fold_in(kz, 1), (), jnp.float32, -1.0, 2.0)
    layers = 2.0 ** jax.random.uniform(kl, (LAYERS, 1, 1), jnp.float32, -1.0, 1.0)
    x = together(ka, jax.random.normal(kx, shape, jnp.float32), much_x) * bump(kf, D, 4.0)
    dy = together(kb, jax.random.normal(kdy, shape, jnp.float32), much_dy)
    drawn = {"x": x.astype(jnp.bfloat16), "dy": (loud * dy * (SEQUENCES * TOKENS) ** -0.5).astype(jnp.bfloat16)}
    for key, name in zip(kw, NAMES, strict=True):
        w = jax.random.normal(key, SHAPES[name], jnp.float32) * SHAPES[name][1] ** -0.5
        drawn[name] = (w * {"w_gate": 1.0, "w_up": bump(kh, FF, 4.0), "w_down": layers}[name]).astype(jnp.bfloat16)
    for key, name in zip(km, NAMES, strict=True):
        drawn[f"m_{name}"] = 0.1 * jax.random.normal(key, SHAPES[name], jnp.float32)
    for key, name in zip(kv, NAMES, strict=True):
        drawn[f"v_{name}"] = jax.random.uniform(key, SHAPES[name], jnp.float32, 0.005, 0.015)
    return drawn


def matmul(a, w):
    return jnp.dot(a, w, preferred_element_type=jnp.float32).astype(jnp.bfloat16)


def normed(h):
    wide = h.astype(jnp.float32)
    scale = lax.rsqrt(jnp.mean(wide**2, -1, keepdims=True) + 1e-6)
    return (wide * scale).astype(jnp.bfloat16)


def layer(h, w):
    a = normed(h)
    gate = jnp.dot(a, w["w_gate"], preferred_element_type=jnp.float32)
    up = jnp.dot(a, w["w_up"], preferred_element_type=jnp.float32)
    return h + matmul((jax.nn.silu(gate) * up).astype(jnp.bfloat16), w["w_down"])


def adamw(w, m, v, g):
    m = 0.9 * m + 0.1 * g
    v = 0.95 * v + 0.05 * g * g
    step = m * lax.rsqrt(v + 1e-8) + 0.1 * w
    return (w - 0.02 * step).astype(jnp.bfloat16), m, v


def clipped(gradients, sum_of_squares, count):
    factor = jnp.minimum(1.0, 0.5 * lax.rsqrt(sum_of_squares / count + 1e-30))
    return [g * factor for g in gradients]


def stack(weights, h):
    return lax.scan(lambda h, w: (layer(h, w), None), h, weights)[0]


def reference(x, dy, w_gate, w_up, w_down, m_w_gate, m_w_up, m_w_down, v_w_gate, v_w_up, v_w_down):
    weights = dict(zip(NAMES, (w_gate, w_up, w_down), strict=True))

    def take(so_far, sequence):
        h, by_y = sequence
        _, back = jax.vjp(lambda w: stack(w, h), weights)
        return jax.tree.map(lambda total, term: total + term.astype(jnp.float32), so_far, back(by_y)[0]), None

    none_yet = {name: jnp.zeros(w.shape, jnp.float32) for name, w in weights.items()}
    by_weights, _ = lax.scan(take, none_yet, (x, dy))
    gradients = [by_weights[name].astype(jnp.bfloat16).astype(jnp.float32) for name in NAMES]
    gradients = clipped(gradients, sum(jnp.sum(g * g) for g in gradients), sum(g.size for g in gradients))
    new = [
        adamw(w.astype(jnp.float32), m, v, g)
        for w, m, v, g in zip((w_gate, w_up, w_down), (m_w_gate, m_w_up, m_w_down), (v_w_gate, v_w_up, v_w_down), gradients, strict=True)
    ]
    return tuple(one[which] for which in range(3) for one in new)
```

```python
import math

import jax
import jax.numpy as jnp
from jax import lax
from jax.experimental import pallas as pl
from jax.experimental.pallas import tpu as pltpu
from jax.sharding import PartitionSpec as P

BF = jnp.bfloat16
F32 = jnp.float32
VMEM_LIMIT = 66_900_000
NN = (((1,), (0,)), ((), ()))
TN = (((0,), (0,)), ((), ()))
NT = (((1,), (1,)), ((), ()))
SIDE = 4
STEP = 640
TOK = 512


def dot(a, b, form):
    return lax.dot_general(a, b, form, preferred_element_type=F32)


def sigmoid(g):
    return 0.5 * jnp.tanh(0.5 * g) + 0.5


def whole(shape):
    return pl.BlockSpec(shape, lambda *_: (0,) * len(shape), pipeline_mode=pl.Buffered(1))


def params(**kw):
    return pltpu.CompilerParams(vmem_limit_bytes=VMEM_LIMIT, **kw)


def norm_rows(h):
    scale = lax.rsqrt(jnp.mean(h * h, 0, keepdims=True) + 1e-6)
    return h * scale


def first_kernel(x_ref, wg_ref, wu_ref, xT_ref, aT_ref, g_ref, u_ref, act_ref):
    tokens = x_ref.shape[0]

    @pl.when(pl.program_id(0) == 0)
    def _():
        def turn(i, _):
            at = pl.ds(pl.multiple_of(i * 128, 128), 128)
            part = x_ref[at, :].astype(F32).T
            xT_ref[:, at] = part.astype(BF)
            aT_ref[:, at] = norm_rows(part).astype(BF)
            return 0

        lax.fori_loop(0, tokens // 128, turn, 0)

    g = dot(wg_ref[...], aT_ref[...], TN)
    g_ref[...] = g
    u = dot(wu_ref[...], aT_ref[...], TN)
    u_ref[...] = u
    act_ref[...] = (g * sigmoid(g) * u).astype(BF)


def first(layer, x, w_gate, w_up):
    tokens, d = x.shape
    ff = w_gate.shape[-1]
    wspec = pl.BlockSpec((None, d, STEP), lambda j: (layer, 0, j))
    hidden = pl.BlockSpec((STEP, tokens), lambda j: (j, 0))
    return pl.pallas_call(
        first_kernel,
        name="first",
        grid=(ff // STEP,),
        in_specs=[whole((tokens, d)), wspec, wspec],
        out_specs=[whole((d, tokens)), whole((d, tokens)), hidden, hidden, hidden],
        out_shape=[
            jax.ShapeDtypeStruct((d, tokens), BF),
            jax.ShapeDtypeStruct((d, tokens), BF),
            jax.ShapeDtypeStruct((ff, tokens), F32),
            jax.ShapeDtypeStruct((ff, tokens), F32),
            jax.ShapeDtypeStruct((ff, tokens), BF),
        ],
        compiler_params=params(),
    )(x, w_gate, w_up)


def down_kernel(wd_ref, act_ref, xT_ref, hT_ref, aT_ref):
    out = dot(wd_ref[...], act_ref[...], TN).astype(BF)
    h = xT_ref[...] + out
    hT_ref[...] = h
    aT_ref[...] = norm_rows(h.astype(F32)).astype(BF)


def down(layer, w_down, act, xT):
    d, tokens = xT.shape
    ff = act.shape[0]
    column = pl.BlockSpec((d, TOK), lambda i: (0, i))
    return pl.pallas_call(
        down_kernel,
        name="down",
        grid=(tokens // TOK,),
        in_specs=[
            pl.BlockSpec((None, ff, d), lambda i: (layer, 0, 0), pipeline_mode=pl.Buffered(1)),
            pl.BlockSpec((ff, TOK), lambda i: (0, i)),
            column,
        ],
        out_specs=[column, column],
        out_shape=[jax.ShapeDtypeStruct((d, tokens), BF)] * 2,
        compiler_params=params(),
    )(w_down, act, xT)


def hidden_back(g, u, da):
    da = da.astype(F32)
    s = sigmoid(g)
    silu = g * s
    return (da * u * (s + silu * (1.0 - s))).astype(BF), (da * silu).astype(BF)


def last_kernel(dy_ref, aT_ref, wg_ref, wu_ref, wd_ref, dyT_ref, act_ref, dgu_ref):
    tokens = dy_ref.shape[0]

    @pl.when(pl.program_id(0) == 0)
    def _():
        def turn(i, _):
            at = pl.ds(pl.multiple_of(i * 128, 128), 128)
            dyT_ref[:, at] = dy_ref[at, :].astype(F32).T.astype(BF)
            return 0

        lax.fori_loop(0, tokens // 128, turn, 0)

    g = dot(wg_ref[...], aT_ref[...], TN)
    u = dot(wu_ref[...], aT_ref[...], TN)
    da = dot(wd_ref[...], dyT_ref[...], NN).astype(BF)
    act_ref[...] = (g * sigmoid(g) * u).astype(BF)
    dgu_ref[0], dgu_ref[1] = hidden_back(g, u, da)


def last(layer, dy, aT, w_gate, w_up, w_down):
    d, tokens = aT.shape
    ff = w_gate.shape[-1]
    wspec = pl.BlockSpec((None, d, STEP), lambda j: (layer, 0, j))
    return pl.pallas_call(
        last_kernel,
        name="last",
        grid=(ff // STEP,),
        in_specs=[whole((tokens, d)), whole((d, tokens)), wspec, wspec, pl.BlockSpec((None, STEP, d), lambda j: (layer, j, 0))],
        out_specs=[
            whole((d, tokens)),
            pl.BlockSpec((STEP, tokens), lambda j: (j, 0)),
            pl.BlockSpec((2, STEP, tokens), lambda j: (0, j, 0)),
        ],
        out_shape=[
            jax.ShapeDtypeStruct((d, tokens), BF),
            jax.ShapeDtypeStruct((ff, tokens), BF),
            jax.ShapeDtypeStruct((2, ff, tokens), BF),
        ],
        compiler_params=params(),
    )(dy, aT, w_gate, w_up, w_down)


def input_kernel(wg_ref, wu_ref, dg_ref, du_ref, hT_ref, dyT_ref, dhT_ref):
    da = dot(wg_ref[...], dg_ref[...], NN).astype(BF) + dot(wu_ref[...], du_ref[...], NN).astype(BF)
    h = hT_ref[...].astype(F32)
    da = da.astype(F32)
    scale = lax.rsqrt(jnp.mean(h * h, 0, keepdims=True) + 1e-6)
    along = jnp.mean(da * h, 0, keepdims=True)
    dh = da * scale - h * (scale * scale * scale * along)
    dhT_ref[...] = dyT_ref[...] + dh.astype(BF)


def back_input(layer, w_gate, w_up, dgu, hT, dyT):
    d, tokens = hT.shape
    ff = w_gate.shape[-1]
    wspec = pl.BlockSpec((None, d, ff), lambda i: (layer, 0, 0), pipeline_mode=pl.Buffered(1))
    column = pl.BlockSpec((d, TOK), lambda i: (0, i))
    return pl.pallas_call(
        input_kernel,
        name="back_input",
        grid=(tokens // TOK,),
        in_specs=[
            wspec,
            wspec,
            pl.BlockSpec((None, ff, TOK), lambda i: (0, 0, i)),
            pl.BlockSpec((None, ff, TOK), lambda i: (1, 0, i)),
            column,
            column,
        ],
        out_specs=column,
        out_shape=jax.ShapeDtypeStruct((d, tokens), BF),
        compiler_params=params(),
    )(w_gate, w_up, dgu, dgu, hT, dyT)


def hidden_kernel(wd_ref, dhT_ref, g_ref, u_ref, dgu_ref):
    da = dot(wd_ref[...], dhT_ref[...], NN).astype(BF)
    dgu_ref[0], dgu_ref[1] = hidden_back(g_ref[...], u_ref[...], da)


def back_hidden(layer, w_down, dhT, g, u):
    d, tokens = dhT.shape
    ff = g.shape[0]
    hidden = pl.BlockSpec((STEP, tokens), lambda j: (j, 0))
    return pl.pallas_call(
        hidden_kernel,
        name="back_hidden",
        grid=(ff // STEP,),
        in_specs=[pl.BlockSpec((None, STEP, d), lambda j: (layer, j, 0)), whole((d, tokens)), hidden, hidden],
        out_specs=pl.BlockSpec((2, STEP, tokens), lambda j: (0, j, 0)),
        out_shape=jax.ShapeDtypeStruct((2, ff, tokens), BF),
        compiler_params=params(),
    )(w_down, dhT, g, u)


OFF_A, OFF_B, OFF_C, OFF_D, OFF_F = 0, 1, 3, 4, 6
N_R0, N_SB, N_RB, N_SC, N_RC, N_SD, N_RD, N_SO = 5, 2, 5, 2, 3, 2, 4, 2
MESH = pl.DeviceIdType.MESH


class Place:
    def __init__(self):
        me = lax.axis_index("dp")
        self.core = me % 2
        self.y = (me // 2) % SIDE
        self.x = me // (2 * SIDE)

    def number(self, x, y, core):
        return ((x % SIDE) * SIDE + y % SIDE) * 2 + core

    def other_core(self):
        return self.number(self.x, self.y, 1 - self.core)

    def first(self, odd):
        return self.x + odd * (self.y - self.x), self.y + odd * (self.x - self.y)

    def along_first(self, odd, by):
        return self.number(self.x + (1 - odd) * by, self.y + odd * by, self.core)

    def along_second(self, odd, by):
        return self.number(self.x + odd * by, self.y + (1 - odd) * by, self.core)


class Reducer:
    def __init__(self, rows, width, slots):
        self.rows, self.width, self.slots = rows, width, slots

    def scratch(self):
        r, w = self.rows, self.width
        dma = pltpu.SemaphoreType.DMA
        return [
            pltpu.VMEM((self.slots, SIDE, SIDE, 2, r, w), BF),
            pltpu.VMEM((N_R0, SIDE, SIDE, r, w), BF),
            pltpu.VMEM((N_SB, 2, 4, r, w), BF),
            pltpu.VMEM((N_RB, 2, 4, r, w), BF),
            pltpu.VMEM((N_SC, 2, 2, r, w), BF),
            pltpu.VMEM((N_RC, 2, 2, r, w), BF),
            pltpu.VMEM((N_SD, 3, r, w), BF),
            pltpu.VMEM((N_RD, 3, r, w), BF),
            pltpu.VMEM((N_SO, r, w), F32),
            dma((self.slots,)),
            dma((N_R0,)),
            dma((N_R0,)),
            dma((N_SB, 2)),
            dma((N_RB, 2)),
            dma((N_SC, 2)),
            dma((N_RC, 2)),
            dma((N_SD, 3)),
            dma((N_RD, 3)),
        ]

    def bind(self, place, refs, finish, load=None):
        self.place, self.finish, self.load = place, finish, load
        (self.G, self.R0, self.SB, self.RB, self.SC, self.RC, self.SD, self.RD, self.SO) = refs[:9]
        (self.l_sem, self.a_send, self.a_recv, self.b_send, self.b_recv, self.c_send, self.c_recv, self.d_send, self.d_recv) = refs[9:]

    def remote(self, src, dst, send, recv, to):
        return pltpu.make_async_remote_copy(src_ref=src, dst_ref=dst, send_sem=send, recv_sem=recv, device_id={"dp": to}, device_id_type=MESH)

    def copy_a(self, k):
        core = self.place.core
        s = k % N_R0
        return self.remote(self.G.at[k % self.slots, :, :, 1 - core], self.R0.at[s], self.a_send.at[s], self.a_recv.at[s], self.place.other_core())

    def copy_b(self, k, way):
        s, r = k % N_SB, k % N_RB
        to = self.place.along_first(k % 2, 1 if way == 0 else SIDE - 1)
        return self.remote(self.SB.at[s, way], self.RB.at[r, way], self.b_send.at[s, way], self.b_recv.at[r, way], to)

    def copy_c(self, k, way):
        s, r = k % N_SC, k % N_RC
        to = self.place.along_first(k % 2, 1 if way == 0 else SIDE - 1)
        return self.remote(self.SC.at[s, way], self.RC.at[r, way], self.c_send.at[s, way], self.c_recv.at[r, way], to)

    def copy_d(self, k, by):
        s, r = k % N_SD, k % N_RD
        to = self.place.along_second(k % 2, by)
        return self.remote(self.SD.at[s, by - 1], self.RD.at[r, by - 1], self.d_send.at[s, by - 1], self.d_recv.at[r, by - 1], to)

    def pair(self, k, target, j):
        odd = k % 2
        x = target + odd * (j - target)
        y = j + odd * (target - j)
        return self.G[k % self.slots, x, y, self.place.core].astype(F32) + self.R0[k % N_R0, x, y].astype(F32)

    def stage_a(self, k):
        if self.load is not None:
            self.load(k, k % self.slots).wait()
        self.copy_a(k).start()

    def stage_b(self, k):
        a = self.copy_a(k)
        a.wait_recv()
        a.wait_send()
        first, _ = self.place.first(k % 2)
        s = k % N_SB
        for way in range(2):
            for j in range(4):
                far = (j < 2) == (way == 0)
                target = (first + (2 if far else 1 if way == 0 else SIDE - 1)) % SIDE
                self.SB[s, way, j] = self.pair(k, target, j).astype(BF)
            self.copy_b(k, way).start()

    def stage_c(self, k):
        first, _ = self.place.first(k % 2)
        s, r = k % N_SC, k % N_RB
        for way in range(2):
            b = self.copy_b(k, way)
            b.wait_send()
            b.wait_recv()
            target = (first + (1 if way == 0 else SIDE - 1)) % SIDE
            for i in range(2):
                j = i + 2 * way
                self.SC[s, way, i] = (self.pair(k, target, j) + self.RB[r, way, j].astype(F32)).astype(BF)
            self.copy_c(k, way).start()

    def stage_d(self, k):
        for way in range(2):
            c = self.copy_c(k, way)
            c.wait_send()
            c.wait_recv()
        first, second = self.place.first(k % 2)
        b, c = k % N_RB, k % N_RC
        for by in (1, 2, 3, 0):
            j = (second + by) % SIDE
            high = j // 2
            total = self.pair(k, first, j) + self.RC[c, high, j % 2].astype(F32) + self.RB[b, 1 - high, j].astype(F32)
            if by:
                self.SD[k % N_SD, by - 1] = total.astype(BF)
                self.copy_d(k, by).start()
            else:
                self.SO[k % N_SO] = total

    def stage_f(self, k):
        total = self.SO[k % N_SO]
        for by in (1, 2, 3):
            d = self.copy_d(k, by)
            d.wait_send()
            d.wait_recv()
            total = total + self.RD[k % N_RD, by - 1].astype(F32)
        self.finish(k, total.astype(BF))

    def tick(self, t, low, high):
        for off, stage in ((OFF_F, self.stage_f), (OFF_D, self.stage_d), (OFF_C, self.stage_c), (OFF_B, self.stage_b), (OFF_A, self.stage_a)):
            k = t - off

            @pl.when(jnp.logical_and(k >= low, k < high))
            def _():
                stage(k)

        if self.load is not None:
            k = t + 1

            @pl.when(jnp.logical_and(k >= low, k < high))
            def _():
                self.load(k, k % self.slots).start()


def weights_kernel(shape, *refs):
    layers, d, ff, tokens, own_gu, own_dn, pad_dn = shape
    ins = refs[: 4 * layers]
    refs = refs[4 * layers :]
    gu_out, dn_out, ssq_out, gdn = refs[:4]
    res, stream, stage, ssq, peer = refs[4:9]
    res_sem, stream_sem, stage_sem, q_send, q_recv = refs[9:14]
    eng = refs[14:]
    place = Place()
    width_gu, width_dn = STEP, 128
    gu_chunks, dn_chunks = 2 * ff // width_gu, d // width_dn
    gu = Reducer(own_gu, width_gu, 7)
    dn = Reducer(pad_dn, width_dn, 5)

    barrier = pltpu.get_barrier_semaphore()
    others = [place.other_core()] + [f(0, by) for by in (1, 2, 3) for f in (place.along_first, place.along_second)]
    for other in others:
        pl.semaphore_signal(barrier, inc=1, device_id={"dp": other}, device_id_type=MESH)
    pl.semaphore_wait(barrier, len(others))

    ssq[...] = jnp.zeros_like(ssq)
    stage[:, :, pad_dn - 8 :, :] = jnp.zeros((2, 4, 8, d), BF)

    def add_squares(g, rows):
        g = g.astype(F32)
        if rows != g.shape[0]:
            g = jnp.where(lax.broadcasted_iota(jnp.int32, g.shape, 0) < rows, g, 0.0)
        g = g * g
        total = g[0:8]
        for i in range(8, g.shape[0], 8):
            total = total + g[i : i + 8]
        lanes = total[:, 0:128]
        for i in range(128, g.shape[1], 128):
            lanes = lanes + total[:, i : i + 128]
        ssq[0] = ssq[0] + lanes

    def finish_gu(k, g):
        gu_out[layers - 1 - k // gu_chunks, :, pl.ds(pl.multiple_of((k % gu_chunks) * width_gu, 128), width_gu)] = g
        add_squares(g, own_gu)

    def finish_dn(k, g):
        dn_out[layers - 1 - k // dn_chunks, :, pl.ds(pl.multiple_of((k % dn_chunks) * width_dn, 128), width_dn)] = g
        add_squares(g, own_dn)

    def load_dn(k, slot):
        at = pl.ds(pl.multiple_of((k % dn_chunks) * width_dn, 128), width_dn)
        return pltpu.make_async_copy(gdn.at[k // dn_chunks, :, :, :, :, at], dn.G.at[slot], dn.l_sem.at[slot])

    n = len(gu.scratch())
    gu.bind(place, eng[:n], finish_gu)
    dn.bind(place, eng[n:], finish_dn, load_dn)

    gu_tile = 2 * STEP
    gu_tiles = 2 * ff // gu_tile
    dn_tile = 4 * own_dn
    dn_tiles = ff // dn_tile

    def stream_gu(layer):
        def copy(i, slot):
            rows = pl.ds(pl.multiple_of(i * gu_tile, 128), gu_tile)
            return pltpu.make_async_copy(ins[4 * layer + 1].at[rows, :], stream.at[slot], stream_sem.at[slot])

        return copy

    def stream_dn(layer):
        def copy(i, slot):
            rows = pl.ds(pl.multiple_of(i * dn_tile, 16), dn_tile)
            return pltpu.make_async_copy(ins[4 * layer + 3].at[rows, :], stream.at[slot, pl.ds(0, dn_tile)], stream_sem.at[slot])

        return copy

    def resident(ref):
        return pltpu.make_async_copy(ref, res, res_sem)

    def compute_gu(first_chunk):
        def run(i, slot, half):
            acc = dot(res[half * (d // 2) : (half + 1) * (d // 2), :], stream[slot], NT)
            for h in range(2):
                at = (first_chunk + 2 * i + h) % gu.slots
                for q in range(SIDE * SIDE):
                    x, y, core = half * 2 + q // (2 * SIDE), (q // 2) % SIDE, q % 2
                    gu.G[at, x, y, core] = acc[q * own_gu : (q + 1) * own_gu, h * STEP : (h + 1) * STEP].astype(BF)

        return run

    def out_dn(layer, i, slot):
        return pltpu.make_async_copy(
            stage.at[slot], gdn.at[layers - 1 - layer, i // 2, pl.ds((i % 2) * 2, 2)].reshape(4, pad_dn, d), stage_sem.at[slot]
        )

    def compute_dn(layer):
        def run(i, slot):
            s = i % 2

            @pl.when(i >= 2)
            def _():
                out_dn(layer, i - 2, s).wait()

            acc = dot(stream[slot, 0:dn_tile, :], res[...], NT)
            for q in range(4):
                stage[s, q, 0:own_dn, :] = acc[q * own_dn : (q + 1) * own_dn].astype(BF)
            out_dn(layer, i, s).start()

        return run

    top = layers - 1
    phases = []
    phases.append(("gu", top, ins[4 * top + 0], gu_tiles, stream_gu(top)))
    for layer in range(top, -1, -1):
        phases.append(("dn", layer, ins[4 * layer + 2], dn_tiles, stream_dn(layer)))
    for layer in range(top - 1, -1, -1):
        phases.append(("gu", layer, ins[4 * layer + 0], gu_tiles, stream_gu(layer)))

    resident(phases[0][2]).start()
    phases[0][4](0, 0).start()
    base = 0
    gu_t, gu_high = 0, 0
    dn_t, dn_low = 0, 0
    lag = OFF_F + 1
    for number, (kind, layer, ref, tiles, copy) in enumerate(phases):
        following = phases[number + 1] if number + 1 < len(phases) else None
        resident(ref).wait()
        gu_first = gu_high
        if kind == "gu":
            gu_high += gu_chunks
            gu_shift = gu_first - 2
        dn_on = number >= 2
        tick_low = 0
        gu_high_now = gu_high
        dn_high = dn_chunks * (min(number - 1, layers)) if dn_on else 0

        def body(i, _, kind=kind, layer=layer, tiles=tiles, copy=copy, base=base, following=following, gu_first=gu_first, dn_t=dn_t, number=number):
            slot = (base + i) % 2
            copy(i, slot).wait()

            @pl.when(i + 1 < tiles)
            def _():
                copy(i + 1, 1 - slot).start()

            if following is not None:

                @pl.when(i + 1 == tiles)
                def _():
                    following[4](0, 1 - slot).start()

            if kind == "gu":
                run = compute_gu(gu_first)
                for half in range(2):
                    if number >= 2:
                        dn.tick(dn_t + 2 * i + half, 0, layers * dn_chunks)
                    gu.tick(gu_first + 2 * i + half - 2, gu_first, gu_first + gu_chunks)
                    run(i, slot, half)
            else:
                if number == 1:
                    gu.tick(gu_chunks - 2 + i, 0, gu_chunks)
                else:
                    dn.tick(dn_t + i, 0, layers * dn_chunks)
                compute_dn(layer)(i, slot)
            return 0

        if number == 2:
            load_dn(0, 0).start()

        lax.fori_loop(0, tiles, body, 0)
        if kind == "dn":
            out_dn(layer, tiles - 2, tiles % 2).wait()
            out_dn(layer, tiles - 1, 1 - tiles % 2).wait()
        if following is not None:
            resident(following[2]).start()
        base += tiles
        if number >= 2:
            dn_t += 2 * tiles if kind == "gu" else tiles

    def drain(i, _):
        dn.tick(dn_t + i, 0, layers * dn_chunks)
        gu.tick(gu_high - 2 + i, gu_high - gu_chunks, gu_high)
        return 0

    lax.fori_loop(0, OFF_F + 2, drain, 0)

    for number, peers in enumerate(([place.other_core()], [place.along_first(0, by) for by in (1, 2, 3)], [place.along_second(0, by) for by in (1, 2, 3)])):
        at = (0, 1, 4)[number]
        copies = []
        for i, to in enumerate(peers):
            copies.append(
                pltpu.make_async_remote_copy(
                    src_ref=ssq.at[number], dst_ref=peer.at[at + i], send_sem=q_send.at[at + i], recv_sem=q_recv.at[at + i], device_id={"dp": to}, device_id_type=MESH
                )
            )
            copies[-1].start()
        total = ssq[number]
        for i, one in enumerate(copies):
            one.wait_recv()
            total = total + peer[at + i]
        for one in copies:
            one.wait_send()
        if number < 2:
            ssq[number + 1] = total
        else:
            ssq_out[...] = total


def weight_gradients(parts, n):
    layers = len(parts)
    d, tokens = parts[0][0].shape
    ff = parts[0][3].shape[0]
    own_gu, own_dn = d // n, ff // n
    pad_dn = -(-own_dn // 8) * 8
    shape = (layers, d, ff, tokens, own_gu, own_dn, pad_dn)
    dma = pltpu.SemaphoreType.DMA
    flat = []
    for aT, dgu, dhT, act in parts:
        flat += [aT, dgu.reshape(2 * ff, tokens), dhT, act]
    vm = pl.BlockSpec(memory_space=pltpu.VMEM)
    hbm = pl.BlockSpec(memory_space=pl.ANY)
    flops = 2 * 3 * layers * d * ff * tokens
    out = pl.pallas_call(
        lambda *refs: weights_kernel(shape, *refs),
        name="weights",
        in_specs=[hbm] * len(flat),
        out_specs=[vm, vm, vm, hbm],
        out_shape=[
            jax.ShapeDtypeStruct((layers, own_gu, 2 * ff), BF),
            jax.ShapeDtypeStruct((layers, pad_dn, d), BF),
            jax.ShapeDtypeStruct((8, 128), F32),
            jax.ShapeDtypeStruct((layers, SIDE, SIDE, 2, pad_dn, d), BF),
        ],
        scratch_shapes=[
            pltpu.VMEM((d, tokens), BF),
            pltpu.VMEM((2, 2 * STEP, tokens), BF),
            pltpu.VMEM((2, 4, pad_dn, d), BF),
            pltpu.VMEM((3, 8, 128), F32),
            pltpu.VMEM((7, 8, 128), F32),
            dma,
            dma((2,)),
            dma((2,)),
            dma((7,)),
            dma((7,)),
        ]
        + Reducer(own_gu, STEP, 7).scratch()
        + Reducer(pad_dn, 128, 5).scratch(),
        compiler_params=params(collective_id=1, has_side_effects=True),
        cost_estimate=pl.CostEstimate(flops=flops, bytes_accessed=2**27, transcendentals=0),
    )(*flat)
    return out[0], out[1][:, :own_dn], jnp.sum(out[2])


def adamw(w, m, v, g):
    m = 0.9 * m + 0.1 * g
    v = 0.95 * v + 0.05 * g * g
    step = m * lax.rsqrt(v + 1e-8) + 0.1 * w
    return (w - 0.02 * step).astype(BF), m, v


def solution(mesh):
    n = mesh.shape["dp"]
    assert n == 2 * SIDE * SIDE and math.isqrt(n // 2) == SIDE

    def one(x, dy, wg, wu, wd, *moments):
        x, dy = x[0], dy[0]
        ff = wg.shape[-1]
        xT, aT0, g0, u0, act0 = first(0, x, wg, wu)
        hT, aT1 = down(0, wd, act0, xT)
        dyT, act1, dgu1 = last(1, dy, aT1, wg, wu, wd)
        dhT = back_input(1, wg, wu, dgu1, hT, dyT)
        dgu0 = back_hidden(0, wd, dhT, g0, u0)
        gu, dn, squares = weight_gradients([(aT0, dgu0, dhT, act0), (aT1, dgu1, dyT, act1)], n)
        count = wg.size + wu.size + wd.size
        factor = jnp.minimum(1.0, 0.5 * lax.rsqrt(squares / count + 1e-30))
        gradients = (gu[:, :, :ff], gu[:, :, ff:], dn)
        me = lax.axis_index("dp")
        ws, ms, vs = [], [], []
        for w, m, v, g in zip((wg, wu, wd), moments[:3], moments[3:], gradients, strict=True):
            mine = lax.dynamic_slice_in_dim(w, me * m.shape[1], m.shape[1], 1)
            w, m, v = adamw(mine.astype(F32), m, v, g.astype(F32) * factor)
            ws.append(lax.all_gather(w, "dp", axis=1, tiled=True))
            ms.append(m)
            vs.append(v)
        return tuple(ws + ms + vs)

    seq = P(("rep", "dp"))
    own = P(None, "dp")
    return jax.shard_map(
        one,
        mesh=mesh,
        in_specs=(seq, seq, P(), P(), P()) + (own,) * 6,
        out_specs=(P("rep"),) * 3 + (P("rep", "dp"),) * 6,
        check_vma=False,
    )
```

```python
import math

import jax
import jax.numpy as jnp
from jax import lax
from jax.experimental import pallas as pl
from jax.experimental.pallas import tpu as pltpu
from jax.sharding import PartitionSpec as P

BF = jnp.bfloat16
F32 = jnp.float32
VMEM_LIMIT = 67_043_328
NN = (((1,), (0,)), ((), ()))
TN = (((0,), (0,)), ((), ()))
NT = (((1,), (1,)), ((), ()))
SIDE = 4
STEP = 640
TOK = 512


def dot(a, b, form):
    return lax.dot_general(a, b, form, preferred_element_type=F32)


def sigmoid(g):
    return 0.5 * jnp.tanh(0.5 * g) + 0.5


def whole(shape):
    return pl.BlockSpec(shape, lambda *_: (0,) * len(shape), pipeline_mode=pl.Buffered(1))


def params(**kw):
    return pltpu.CompilerParams(vmem_limit_bytes=VMEM_LIMIT, **kw)


def norm_rows(h):
    scale = lax.rsqrt(jnp.mean(h * h, 0, keepdims=True) + 1e-6)
    return h * scale


def first_kernel(x_ref, wg_ref, wu_ref, xT_ref, aT_ref, g_ref, u_ref, act_ref):
    tokens = x_ref.shape[0]

    @pl.when(pl.program_id(0) == 0)
    def _():
        def turn(i, _):
            at = pl.ds(pl.multiple_of(i * 128, 128), 128)
            part = x_ref[at, :].astype(F32).T
            xT_ref[:, at] = part.astype(BF)
            aT_ref[:, at] = norm_rows(part).astype(BF)
            return 0

        lax.fori_loop(0, tokens // 128, turn, 0)

    g = dot(wg_ref[...], aT_ref[...], TN)
    g_ref[...] = g
    u = dot(wu_ref[...], aT_ref[...], TN)
    u_ref[...] = u
    act_ref[...] = (g * sigmoid(g) * u).astype(BF)


def first(layer, x, w_gate, w_up):
    tokens, d = x.shape
    ff = w_gate.shape[-1]
    wspec = pl.BlockSpec((None, d, STEP), lambda j: (layer, 0, j))
    hidden = pl.BlockSpec((STEP, tokens), lambda j: (j, 0))
    return pl.pallas_call(
        first_kernel,
        name="first",
        grid=(ff // STEP,),
        in_specs=[whole((tokens, d)), wspec, wspec],
        out_specs=[whole((d, tokens)), whole((d, tokens)), hidden, hidden, hidden],
        out_shape=[
            jax.ShapeDtypeStruct((d, tokens), BF),
            jax.ShapeDtypeStruct((d, tokens), BF),
            jax.ShapeDtypeStruct((ff, tokens), F32),
            jax.ShapeDtypeStruct((ff, tokens), F32),
            jax.ShapeDtypeStruct((ff, tokens), BF),
        ],
        compiler_params=params(),
    )(x, w_gate, w_up)


def down_kernel(wd_ref, act_ref, xT_ref, hT_ref, aT_ref):
    out = dot(wd_ref[...], act_ref[...], TN).astype(BF)
    h = xT_ref[...] + out
    hT_ref[...] = h
    aT_ref[...] = norm_rows(h.astype(F32)).astype(BF)


def down(layer, w_down, act, xT):
    d, tokens = xT.shape
    ff = act.shape[0]
    column = pl.BlockSpec((d, TOK), lambda i: (0, i))
    return pl.pallas_call(
        down_kernel,
        name="down",
        grid=(tokens // TOK,),
        in_specs=[
            pl.BlockSpec((None, ff, d), lambda i: (layer, 0, 0), pipeline_mode=pl.Buffered(1)),
            pl.BlockSpec((ff, TOK), lambda i: (0, i)),
            column,
        ],
        out_specs=[column, column],
        out_shape=[jax.ShapeDtypeStruct((d, tokens), BF)] * 2,
        compiler_params=params(),
    )(w_down, act, xT)


def hidden_back(g, u, da):
    da = da.astype(F32)
    s = sigmoid(g)
    silu = g * s
    return (da * u * (s + silu * (1.0 - s))).astype(BF), (da * silu).astype(BF)


def last_kernel(dy_ref, aT_ref, wg_ref, wu_ref, wd_ref, dyT_ref, act_ref, dgu_ref):
    tokens = dy_ref.shape[0]

    @pl.when(pl.program_id(0) == 0)
    def _():
        def turn(i, _):
            at = pl.ds(pl.multiple_of(i * 128, 128), 128)
            dyT_ref[:, at] = dy_ref[at, :].astype(F32).T.astype(BF)
            return 0

        lax.fori_loop(0, tokens // 128, turn, 0)

    g = dot(wg_ref[...], aT_ref[...], TN)
    u = dot(wu_ref[...], aT_ref[...], TN)
    da = dot(wd_ref[...], dyT_ref[...], NN).astype(BF)
    act_ref[...] = (g * sigmoid(g) * u).astype(BF)
    dgu_ref[0], dgu_ref[1] = hidden_back(g, u, da)


def last(layer, dy, aT, w_gate, w_up, w_down):
    d, tokens = aT.shape
    ff = w_gate.shape[-1]
    wspec = pl.BlockSpec((None, d, STEP), lambda j: (layer, 0, j))
    return pl.pallas_call(
        last_kernel,
        name="last",
        grid=(ff // STEP,),
        in_specs=[whole((tokens, d)), whole((d, tokens)), wspec, wspec, pl.BlockSpec((None, STEP, d), lambda j: (layer, j, 0))],
        out_specs=[
            whole((d, tokens)),
            pl.BlockSpec((STEP, tokens), lambda j: (j, 0)),
            pl.BlockSpec((None, 2, STEP, tokens), lambda j: (j, 0, 0, 0)),
        ],
        out_shape=[
            jax.ShapeDtypeStruct((d, tokens), BF),
            jax.ShapeDtypeStruct((ff, tokens), BF),
            jax.ShapeDtypeStruct((ff // STEP, 2, STEP, tokens), BF),
        ],
        compiler_params=params(),
    )(dy, aT, w_gate, w_up, w_down)


OFF_A, OFF_B, OFF_C, OFF_D, OFF_F = 0, 1, 3, 5, 7
N_G, N_R0, N_SB, N_RB, N_SC, N_RC, N_SD, N_RD, N_SO = 8, 6, 2, 6, 2, 4, 2, 4, 2
WIDE = STEP
MESH = pl.DeviceIdType.MESH


class Place:
    def __init__(self):
        me = lax.axis_index("dp")
        self.core = me % 2
        self.y = (me // 2) % SIDE
        self.x = me // (2 * SIDE)

    def number(self, x, y, core):
        return ((x % SIDE) * SIDE + y % SIDE) * 2 + core

    def other_core(self):
        return self.number(self.x, self.y, 1 - self.core)

    def first(self, odd):
        return self.x + odd * (self.y - self.x), self.y + odd * (self.x - self.y)

    def along_first(self, odd, by):
        return self.number(self.x + (1 - odd) * by, self.y + odd * by, self.core)

    def along_second(self, odd, by):
        return self.number(self.x + odd * by, self.y + (1 - odd) * by, self.core)

    def meet(self):
        barrier = pltpu.get_barrier_semaphore()
        others = [self.other_core()] + [f(0, by) for by in (1, 2, 3) for f in (self.along_first, self.along_second)]
        for other in others:
            pl.semaphore_signal(barrier, inc=1, device_id={"dp": other}, device_id_type=MESH)
        pl.semaphore_wait(barrier, len(others))


class Reducer:
    @staticmethod
    def scratch(r, w):
        dma = pltpu.SemaphoreType.DMA
        return [
            pltpu.VMEM((N_G, SIDE, SIDE, 2, r, w), BF),
            pltpu.VMEM((N_R0, SIDE, SIDE, r, w), BF),
            pltpu.VMEM((N_SB, 2, 4, r, w), BF),
            pltpu.VMEM((N_RB, 2, 4, r, w), BF),
            pltpu.VMEM((N_SC, 2, 2, r, w), BF),
            pltpu.VMEM((N_RC, 2, 2, r, w), BF),
            pltpu.VMEM((N_SD, 3, r, w), BF),
            pltpu.VMEM((N_RD, 3, r, w), BF),
            pltpu.VMEM((N_SO, r, w), F32),
            dma((N_G,)),
            dma((N_R0,)),
            dma((N_R0,)),
            dma((N_SB, 2)),
            dma((N_RB, 2)),
            dma((N_SC, 2)),
            dma((N_RC, 2)),
            dma((N_SD, 3)),
            dma((N_RD, 3)),
        ]

    def __init__(self, place, refs, finish):
        self.place, self.finish = place, finish
        (self.G, self.R0, self.SB, self.RB, self.SC, self.RC, self.SD, self.RD, self.SO) = refs[:9]
        (self.l_sem, self.a_send, self.a_recv, self.b_send, self.b_recv, self.c_send, self.c_recv, self.d_send, self.d_recv) = refs[9:]

    def remote(self, src, dst, send, recv, to):
        return pltpu.make_async_remote_copy(src_ref=src, dst_ref=dst, send_sem=send, recv_sem=recv, device_id={"dp": to}, device_id_type=MESH)

    def copy_a(self, k):
        s = k % N_R0
        return self.remote(self.G.at[k % N_G, :, :, 1 - self.place.core], self.R0.at[s], self.a_send.at[s], self.a_recv.at[s], self.place.other_core())

    def copy_b(self, k, way):
        s, r = k % N_SB, k % N_RB
        to = self.place.along_first(k % 2, 1 if way == 0 else SIDE - 1)
        return self.remote(self.SB.at[s, way], self.RB.at[r, way], self.b_send.at[s, way], self.b_recv.at[r, way], to)

    def copy_c(self, k, way):
        s, r = k % N_SC, k % N_RC
        to = self.place.along_first(k % 2, 1 if way == 0 else SIDE - 1)
        return self.remote(self.SC.at[s, way], self.RC.at[r, way], self.c_send.at[s, way], self.c_recv.at[r, way], to)

    def copy_d(self, k, by):
        s, r = k % N_SD, k % N_RD
        to = self.place.along_second(k % 2, by)
        return self.remote(self.SD.at[s, by - 1], self.RD.at[r, by - 1], self.d_send.at[s, by - 1], self.d_recv.at[r, by - 1], to)

    def pair(self, k, target, j):
        odd = k % 2
        x = target + odd * (j - target)
        y = j + odd * (target - j)
        return self.G[k % N_G, x, y, self.place.core].astype(F32) + self.R0[k % N_R0, x, y].astype(F32)

    def stage_a(self, k):
        self.copy_a(k).start()

    def stage_b(self, k):
        a = self.copy_a(k)
        a.wait_recv()
        a.wait_send()
        first, _ = self.place.first(k % 2)
        s = k % N_SB
        for way in range(2):
            for j in range(4):
                far = (j < 2) == (way == 0)
                target = (first + (2 if far else 1 if way == 0 else SIDE - 1)) % SIDE
                self.SB[s, way, j] = self.pair(k, target, j).astype(BF)
            self.copy_b(k, way).start()

    def stage_c(self, k):
        first, _ = self.place.first(k % 2)
        s, r = k % N_SC, k % N_RB
        for way in range(2):
            b = self.copy_b(k, way)
            b.wait_send()
            b.wait_recv()
            target = (first + (1 if way == 0 else SIDE - 1)) % SIDE
            for i in range(2):
                j = i + 2 * way
                self.SC[s, way, i] = (self.pair(k, target, j) + self.RB[r, way, j].astype(F32)).astype(BF)
            self.copy_c(k, way).start()

    def stage_d(self, k):
        for way in range(2):
            c = self.copy_c(k, way)
            c.wait_send()
            c.wait_recv()
        first, second = self.place.first(k % 2)
        b, c = k % N_RB, k % N_RC
        for by in (1, 2, 3, 0):
            j = (second + by) % SIDE
            high = j // 2
            total = self.pair(k, first, j) + self.RC[c, high, j % 2].astype(F32) + self.RB[b, 1 - high, j].astype(F32)
            if by:
                self.SD[k % N_SD, by - 1] = total.astype(BF)
                self.copy_d(k, by).start()
            else:
                self.SO[k % N_SO] = total

    def stage_f(self, k):
        total = self.SO[k % N_SO]
        for by in (1, 2, 3):
            d = self.copy_d(k, by)
            d.wait_send()
            d.wait_recv()
            total = total + self.RD[k % N_RD, by - 1].astype(F32)
        self.finish(k, total.astype(BF))

    def tick(self, t, low, high, load=None):
        for off, stage in ((OFF_F, self.stage_f), (OFF_D, self.stage_d), (OFF_C, self.stage_c), (OFF_B, self.stage_b), (OFF_A, self.stage_a)):
            k = t - off
            if isinstance(k, int):
                if low <= k < high:
                    stage(k)
                continue

            @pl.when(jnp.logical_and(k >= low, k < high))
            def _():
                if off == OFF_A and load is not None:
                    load(k).wait()
                stage(k)


def weights_kernel(shape, *refs):
    d, ff, tokens, own_gu, own_dn, packs = shape
    (aT0, act0, g0, u0, wd, hT, aT1, act1, dgu1, dyT, wg, wu) = refs[:12]
    out, ssq_out, gdn = refs[12:15]
    res, stream, acc, wbuf, stage, ready, ssq, peer = refs[15:23]
    res_sem, stream_sem, acc_sem, w_sem, stage_sem, ready_sem, q_send, q_recv = refs[23:31]
    place = Place()
    tiles = ff // STEP
    half = d // 2
    assert half == STEP
    dn_tile = 4 * own_dn
    dn_tiles = ff // dn_tile
    layer_chunks = 3 * tiles
    assert packs == tiles and packs <= dn_tiles

    place.meet()
    ssq[...] = jnp.zeros_like(ssq)

    def put(k):
        return pltpu.make_async_copy(ready.at[k % 2], out.at[k], ready_sem.at[k % 2])

    def finish(k, g):
        @pl.when(k >= 2)
        def _():
            put(k - 2).wait()

        ready[k % 2] = g
        put(k).start()
        g = g.astype(F32)
        g = g * g
        rows = g[0:8]
        for i in range(8, g.shape[0], 8):
            rows = rows + g[i : i + 8]
        lanes = rows[:, 0:128]
        for i in range(128, g.shape[1], 128):
            lanes = lanes + rows[:, i : i + 128]
        ssq[0] = ssq[0] + lanes

    eng = Reducer(place, refs[31:], finish)

    def copy(src, dst, sem):
        return pltpu.make_async_copy(src, dst, sem)

    def rows(i, size):
        return pl.ds(pl.multiple_of(i * size, 16), size)

    def load_res(which, ref):
        return copy(ref, res.at[which], res_sem.at[which])

    def stream_gu(i, slot):
        return copy(dgu1.at[i], stream.at[slot], stream_sem.at[slot])

    def stream_dn(ref, i, slot):
        return copy(ref.at[rows(i, dn_tile), :], stream.at[slot, pl.ds(0, dn_tile)], stream_sem.at[slot])

    def w_tile(i, part):
        at = pl.ds(pl.multiple_of(i * STEP, 128), STEP)
        return [copy(w.at[1, pl.ds(part * half, half), at], wbuf.at[:, pl.ds(n * STEP, STEP)], w_sem.at[n]) for n, w in enumerate((wg, wu))]

    def hidden_tile(i):
        return [
            copy(g0.at[rows(i, STEP), :], acc.at[pl.ds(0, STEP)], acc_sem.at[0]),
            copy(u0.at[rows(i, STEP), :], acc.at[pl.ds(STEP, STEP)], acc_sem.at[1]),
            copy(wd.at[0, rows(i, STEP), :], wbuf, w_sem.at[0]),
        ]

    def wgrad(which, slot, part, first):
        product = dot(res[which, part * half : (part + 1) * half, :], stream[slot], NT)
        for c in range(2):
            for q in range(SIDE * SIDE):
                x, y, core = part * 2 + q // (2 * SIDE), (q // 2) % SIDE, q % 2
                eng.G[(first + c) % N_G, x, y, core] = product[q * own_gu : (q + 1) * own_gu, c * WIDE : (c + 1) * WIDE].astype(BF)

    stage[...] = jnp.zeros_like(stage)
    full = own_dn // own_gu
    rest = own_dn - full * own_gu
    blocks = d // WIDE

    def out_dn(number, i, s):
        return copy(stage.at[s], gdn.at[number, :, i // 2, pl.ds((i % 2) * 2, 2)], stage_sem.at[s])

    def load_dn(number, chunk, k):
        return copy(gdn.at[number, chunk], eng.G.at[k % N_G], eng.l_sem.at[k % N_G])

    def down_gradient(number, which, i, slot):
        s = i % 2

        @pl.when(i >= 2)
        def _():
            out_dn(number, i - 2, s).wait()

        product = dot(stream[slot, 0:dn_tile, :], res[which], NT)
        for q in range(4):
            for b in range(blocks):
                lanes = slice(b * WIDE, (b + 1) * WIDE)
                for p in range(full):
                    r = q * own_dn + p * own_gu
                    stage[s, p * blocks + b, q // 2, q % 2] = product[r : r + own_gu, lanes].astype(BF)
                r = q * own_dn + full * own_gu
                stage[s, full * blocks + b // 2, q // 2, q % 2, (b % 2) * rest : (b % 2 + 1) * rest] = product[r : r + rest, lanes].astype(BF)
        out_dn(number, i, s).start()

    load_res(1, dyT).start()
    stream_dn(act1, 0, 0).start()
    load_res(0, aT1).start()
    for one in w_tile(0, 0):
        one.start()
    acc[...] = jnp.zeros_like(acc)
    load_res(1, dyT).wait()

    def down1(i, _):
        slot = i % 2
        stream_dn(act1, i, slot).wait()

        @pl.when(i + 1 < dn_tiles)
        def _():
            stream_dn(act1, i + 1, 1 - slot).start()

        @pl.when(i + 1 == dn_tiles)
        def _():
            stream_gu(0, 1 - slot).start()

        down_gradient(0, 1, i, slot)
        return 0

    lax.fori_loop(0, dn_tiles, down1, 0)
    for i in range(dn_tiles - 2, dn_tiles):
        out_dn(0, i, i % 2).wait()
    load_dn(0, 0, 0).start()
    load_res(0, aT1).wait()

    def layer1(i, _):
        slot = (dn_tiles + i) % 2
        load = lambda k: load_dn(0, k // 3, k)
        stream_gu(i, slot).wait()

        @pl.when(i + 1 < tiles)
        def _():
            stream_gu(i + 1, 1 - slot).start()

        @pl.when(i + 1 == tiles)
        def _():
            copy(hT, stream.at[1 - slot], stream_sem.at[1 - slot]).start()

        wgrad(0, slot, 0, 3 * i + 1)
        eng.tick(3 * i, 0, layer_chunks, load)

        @pl.when(i + 1 < tiles)
        def _():
            load(3 * i + 3).start()

        for part in range(2):
            if part:
                wgrad(0, slot, 1, 3 * i + 1)
                eng.tick(3 * i + 1, 0, layer_chunks)
            for one in w_tile(i, part):
                one.wait()
            acc[part * half : (part + 1) * half] += dot(wbuf[...], stream[slot], NN)
            if not part:
                for one in w_tile(i, 1):
                    one.start()

        @pl.when(i + 1 < tiles)
        def _():
            for one in w_tile(i + 1, 0):
                one.start()

        eng.tick(3 * i + 2, 0, layer_chunks)
        return 0

    lax.fori_loop(0, tiles, layer1, 0)

    s_h = (dn_tiles + tiles) % 2
    stream_dn(act0, 0, 1 - s_h).start()
    copy(hT, stream.at[s_h], stream_sem.at[s_h]).wait()

    def back_norm(i, _):
        at = pl.ds(pl.multiple_of(i * 128, 128), 128)
        h = stream[s_h, :, at].astype(F32)
        da = acc[:, at].astype(BF).astype(F32)
        scale = lax.rsqrt(jnp.mean(h * h, 0, keepdims=True) + 1e-6)
        along = jnp.mean(da * h, 0, keepdims=True)
        dh = da * scale - h * (scale * scale * scale * along)
        res[0, :, at] = res[1, :, at] + dh.astype(BF)
        return 0

    lax.fori_loop(0, tokens // 128, back_norm, 0)
    for one in hidden_tile(0):
        one.start()
    load_res(1, aT0).start()

    def down0(i, _):
        slot = (1 - s_h + i) % 2
        stream_dn(act0, i, slot).wait()

        @pl.when(i + 1 < dn_tiles)
        def _():
            stream_dn(act0, i + 1, 1 - slot).start()

        eng.tick(layer_chunks + i, 0, layer_chunks)
        down_gradient(1, 0, i, slot)
        return 0

    assert dn_tiles >= OFF_F
    lax.fori_loop(0, dn_tiles, down0, 0)
    for i in range(dn_tiles - 2, dn_tiles):
        out_dn(1, i, i % 2).wait()
    load_dn(1, 0, layer_chunks).start()
    load_res(1, aT0).wait()

    def layer0(i, _):
        base = layer_chunks + 3 * i
        load = lambda k: load_dn(1, k // 3 - tiles, k)

        @pl.when(i > 0)
        def _():
            eng.tick(base - 2, layer_chunks, 2 * layer_chunks)

        for one in hidden_tile(i):
            one.wait()
        for part in range(2):
            at = pl.ds(part * (tokens // 2), tokens // 2)
            da = dot(wbuf[...], res[0, :, at], NN).astype(BF)
            stream[0, 0:STEP, at], stream[0, STEP:, at] = hidden_back(acc[0:STEP, at], acc[STEP:, at], da)

        @pl.when(i > 0)
        def _():
            eng.tick(base - 1, layer_chunks, 2 * layer_chunks)
            load(base).start()

        @pl.when(i + 1 < tiles)
        def _():
            for one in hidden_tile(i + 1):
                one.start()

        wgrad(1, 0, 0, base + 1)
        eng.tick(base, layer_chunks, 2 * layer_chunks, load)
        wgrad(1, 0, 1, base + 1)
        return 0

    lax.fori_loop(0, tiles, layer0, 0)

    def drain(i, _):
        eng.tick(2 * layer_chunks - 2 + i, layer_chunks, 2 * layer_chunks)
        return 0

    lax.fori_loop(0, 2 + OFF_F, drain, 0)
    for k in range(2 * layer_chunks - 2, 2 * layer_chunks):
        put(k).wait()

    for number, peers in enumerate(([place.other_core()], [place.along_first(0, by) for by in (1, 2, 3)], [place.along_second(0, by) for by in (1, 2, 3)])):
        at = (0, 1, 4)[number]
        copies = []
        for i, to in enumerate(peers):
            copies.append(eng.remote(ssq.at[number], peer.at[at + i], q_send.at[at + i], q_recv.at[at + i], to))
            copies[-1].start()
        total = ssq[number]
        for i, one in enumerate(copies):
            one.wait_recv()
            total = total + peer[at + i]
        for one in copies:
            one.wait_send()
        if number < 2:
            ssq[number + 1] = total
        else:
            ssq_out[...] = total


def weight_gradients(aT0, act0, g0, u0, wd, hT, aT1, act1, dgu1, dyT, wg, wu, n):
    d, tokens = aT0.shape
    ff = act0.shape[0]
    tiles = ff // STEP
    own_gu, own_dn = d // n, ff // n
    blocks = d // WIDE
    full = own_dn // own_gu
    rest = own_dn - full * own_gu
    assert 2 * rest <= own_gu
    packs = full * blocks + -(-blocks // 2)
    dma = pltpu.SemaphoreType.DMA
    flat = (aT0, act0, g0, u0, wd, hT, aT1, act1, dgu1.reshape(tiles, 2 * STEP, tokens), dyT, wg, wu)
    vm = pl.BlockSpec(memory_space=pltpu.VMEM)
    hbm = pl.BlockSpec(memory_space=pl.ANY)
    layer_chunks = 3 * tiles
    out, squares, _ = pl.pallas_call(
        lambda *refs: weights_kernel((d, ff, tokens, own_gu, own_dn, packs), *refs),
        name="weights",
        in_specs=[hbm] * len(flat),
        out_specs=[hbm, vm, hbm],
        out_shape=[
            jax.ShapeDtypeStruct((2 * layer_chunks, own_gu, WIDE), BF),
            jax.ShapeDtypeStruct((8, 128), F32),
            jax.ShapeDtypeStruct((2, packs, SIDE, SIDE, 2, own_gu, WIDE), BF),
        ],
        scratch_shapes=[
            pltpu.VMEM((2, d, tokens), BF),
            pltpu.VMEM((2, 2 * STEP, tokens), BF),
            pltpu.VMEM((d, tokens), F32),
            pltpu.VMEM((STEP, d), BF),
            pltpu.VMEM((2, packs, 2, 2, own_gu, WIDE), BF),
            pltpu.VMEM((2, own_gu, WIDE), BF),
            pltpu.VMEM((3, 8, 128), F32),
            pltpu.VMEM((7, 8, 128), F32),
            dma((2,)),
            dma((2,)),
            dma((2,)),
            dma((2,)),
            dma((2,)),
            dma((2,)),
            dma((7,)),
            dma((7,)),
        ]
        + Reducer.scratch(own_gu, WIDE),
        compiler_params=params(collective_id=1, has_side_effects=True),
        cost_estimate=pl.CostEstimate(flops=18 * d * ff * tokens, bytes_accessed=2**27, transcendentals=0),
    )(*flat)
    layers = []
    for number in (1, 0):
        chunks = out[number * layer_chunks : (number + 1) * layer_chunks].reshape(tiles, 3, own_gu, WIDE)
        dn = chunks[:, 0]
        gu = chunks[:, 1:].transpose(1, 2, 0, 3).reshape(2, own_gu, ff)
        top = dn[: full * blocks].reshape(full, blocks, own_gu, WIDE).transpose(0, 2, 1, 3).reshape(full * own_gu, d)
        low = dn[full * blocks :, : 2 * rest].reshape(-1, rest, WIDE)[:blocks].transpose(1, 0, 2).reshape(rest, d)
        layers.append((gu[0], gu[1], jnp.concatenate([top, low])))
    return [jnp.stack(one) for one in zip(*layers)], jnp.sum(squares)


def gather_kernel(own_ref, out_ref, land, own_sem, out_sem, send, recv):
    place = Place()
    me = place.number(place.x, place.y, place.core)
    mine = pltpu.make_async_copy(own_ref, land.at[:, me], own_sem)
    mine.start()
    place.meet()
    mine.wait()
    started = []

    def at(half, first, second, core=None):
        x, y = (first, second) if half == 0 else (second, first)
        return place.number(place.x + x, place.y + y, place.core if core is None else core)

    def copy(half, number, slot, to):
        strip = land.at[half, number]
        return pltpu.make_async_remote_copy(
            src_ref=strip, dst_ref=strip, send_sem=send.at[half, slot], recv_sem=recv.at[half, slot], device_id={"dp": to}, device_id_type=MESH
        )

    def go(*what):
        started.append(copy(*what))
        started[-1].start()

    def from_side(first, way):
        return 3 + 2 * first + way

    def from_far(first):
        return 11 + first

    def from_core(first, second):
        return 15 + 4 * first + second

    sides = (1, 3)
    for half in range(2):
        for by in (1, 3, 2):
            go(half, me, by - 1, at(half, by, 0))
    for half in range(2):
        for way in range(2):
            go(half, me, from_side(0, way), at(half, 0, sides[way]))
    for half in range(2):
        go(half, me, from_core(0, 0), place.other_core())
    for by in (1, 3, 2):
        for half in range(2):
            first = SIDE - by
            owner = at(half, first, 0)
            copy(half, owner, by - 1, me).wait_recv()
            for way in range(2):
                go(half, owner, from_side(first, way), at(half, 0, sides[way]))
            go(half, owner, from_core(first, 0), place.other_core())
    for first in (0, 3, 1, 2):
        for half in range(2):
            for way in range(2):
                second = SIDE - sides[way]
                owner = at(half, first, second)
                copy(half, owner, from_side(first, way), me).wait_recv()
                if (first < 2) == (way == 0):
                    go(half, owner, from_far(first), at(half, 0, sides[way]))
                go(half, owner, from_core(first, second), place.other_core())
    for first in (0, 3, 1, 2):
        for half in range(2):
            owner = at(half, first, 2)
            copy(half, owner, from_far(first), me).wait_recv()
            go(half, owner, from_core(first, 2), place.other_core())
    for first in range(SIDE):
        for second in range(SIDE):
            for half in range(2):
                copy(half, at(half, first, second, 1 - place.core), from_core(first, second), me).wait_recv()
    outs = []
    each = land.shape[1] // 8
    for i in range(8):
        part = pl.ds(i * each, each)
        outs.append(pltpu.make_async_copy(land.at[:, part], out_ref.at[:, part], out_sem.at[i]))
        outs[-1].start()
    for one in started:
        one.wait_send()
    for one in outs:
        one.wait()


def gather(own, n):
    layers, rows, columns = own.shape
    assert layers == 2
    dma = pltpu.SemaphoreType.DMA
    slots = 15 + SIDE * SIDE
    size = 2 * own.size * n
    out = pl.pallas_call(
        gather_kernel,
        name="gather",
        in_specs=[pl.BlockSpec(memory_space=pl.ANY)],
        out_specs=pl.BlockSpec(memory_space=pl.ANY),
        out_shape=jax.ShapeDtypeStruct((layers, n, rows, columns), BF),
        scratch_shapes=[pltpu.VMEM((layers, n, rows, columns), BF), dma, dma((8,)), dma((2, slots)), dma((2, slots))],
        compiler_params=pltpu.CompilerParams(vmem_limit_bytes=size + 2**21, collective_id=2, has_side_effects=True),
        cost_estimate=pl.CostEstimate(flops=10**11, bytes_accessed=size, transcendentals=0),
    )(own)
    return out.reshape(layers, n * rows, columns)


def settle_kernel(in_ref, out_ref):
    out_ref[...] = in_ref[...]


def settle(w):
    layers, rows, columns = w.shape
    block = pl.BlockSpec((None, 320, columns), lambda i, j: (i, j, 0))
    return pl.pallas_call(
        settle_kernel,
        name="settle",
        grid=(layers, rows // 320),
        in_specs=[block],
        out_specs=block,
        out_shape=jax.ShapeDtypeStruct(w.shape, BF),
        compiler_params=pltpu.CompilerParams(vmem_limit_bytes=2**24),
        cost_estimate=pl.CostEstimate(flops=10**10, bytes_accessed=4 * w.size, transcendentals=0),
    )(w)


def join_kernel(in_ref, out_ref, wide):
    strips, rows, _ = in_ref.shape
    for i in range(strips):
        wide[i * rows : (i + 1) * rows, :] = in_ref[i].astype(F32)
    out_ref[...] = wide[...].astype(BF)


def join(parts):
    n, layers, rows, columns = parts.shape
    size = 4 * rows
    return pl.pallas_call(
        join_kernel,
        name="join",
        grid=(layers, n // 4),
        in_specs=[pl.BlockSpec((4, None, rows, columns), lambda i, j: (j, i, 0, 0))],
        out_specs=pl.BlockSpec((None, size, columns), lambda i, j: (i, j, 0)),
        out_shape=jax.ShapeDtypeStruct((layers, n * rows, columns), BF),
        scratch_shapes=[pltpu.VMEM((size, columns), F32)],
        compiler_params=pltpu.CompilerParams(vmem_limit_bytes=2**24),
        cost_estimate=pl.CostEstimate(flops=10**10, bytes_accessed=4 * parts.size, transcendentals=0),
    )(parts)


def adamw(w, m, v, g):
    m = 0.9 * m + 0.1 * g
    v = 0.95 * v + 0.05 * g * g
    step = m * lax.rsqrt(v + 1e-8) + 0.1 * w
    return (w - 0.02 * step).astype(BF), m, v


def solution(mesh):
    n = mesh.shape["dp"]
    assert n == 2 * SIDE * SIDE and math.isqrt(n // 2) == SIDE

    def one(x, dy, wg, wu, wd, *moments):
        x, dy = x[0], dy[0]
        xT, aT0, g0, u0, act0 = first(0, x, wg, wu)
        hT, aT1 = down(0, wd, act0, xT)
        dyT, act1, dgu1 = last(1, dy, aT1, wg, wu, wd)
        gradients, squares = weight_gradients(aT0, act0, g0, u0, wd, hT, aT1, act1, dgu1, dyT, wg, wu, n)
        count = wg.size + wu.size + wd.size
        factor = jnp.minimum(1.0, 0.5 * lax.rsqrt(squares / count + 1e-30))
        me = lax.axis_index("dp")
        ws, ms, vs = [], [], []
        for w, m, v, g in zip((wg, wu, wd), moments[:3], moments[3:], gradients, strict=True):
            mine = lax.dynamic_slice_in_dim(w, me * m.shape[1], m.shape[1], 1)
            w, m, v = adamw(mine.astype(F32), m, v, g.astype(F32) * factor)
            ws.append(w)
            ms.append(m)
            vs.append(v)
        new_down = join(lax.all_gather(ws[2], "dp", axis=0))
        new_up = settle(lax.all_gather(ws[1], "dp", axis=1, tiled=True))
        new_gate = settle(gather(ws[0], n))
        return (new_gate, new_up, new_down, *ms, *vs)

    seq = P(("rep", "dp"))
    own = P(None, "dp")
    return jax.shard_map(
        one,
        mesh=mesh,
        in_specs=(seq, seq, P(), P(), P()) + (own,) * 6,
        out_specs=(P("rep"),) * 3 + (P("rep", "dp"),) * 6,
        check_vma=False,
    )
```

```python
import math

import jax
import jax.numpy as jnp
from jax import lax
from jax.experimental import pallas as pl
from jax.experimental.pallas import tpu as pltpu
from jax.sharding import PartitionSpec as P

BF = jnp.bfloat16
F32 = jnp.float32
VMEM_LIMIT = 67_043_328
NN = (((1,), (0,)), ((), ()))
TN = (((0,), (0,)), ((), ()))
NT = (((1,), (1,)), ((), ()))
SIDE = 4
STEP = 640
TOK = 512


def dot(a, b, form):
    return lax.dot_general(a, b, form, preferred_element_type=F32)


def sigmoid(g):
    return 0.5 * jnp.tanh(0.5 * g) + 0.5


def whole(shape):
    return pl.BlockSpec(shape, lambda *_: (0,) * len(shape), pipeline_mode=pl.Buffered(1))


def params(**kw):
    return pltpu.CompilerParams(vmem_limit_bytes=VMEM_LIMIT, **kw)


def norm_rows(h):
    scale = lax.rsqrt(jnp.mean(h * h, 0, keepdims=True) + 1e-6)
    return h * scale


def first_kernel(x_ref, wg_ref, wu_ref, xT_ref, aT_ref, g_ref, u_ref, act_ref):
    tokens = x_ref.shape[0]

    @pl.when(pl.program_id(0) == 0)
    def _():
        def turn(i, _):
            at = pl.ds(pl.multiple_of(i * 128, 128), 128)
            part = x_ref[at, :].astype(F32).T
            xT_ref[:, at] = part.astype(BF)
            aT_ref[:, at] = norm_rows(part).astype(BF)
            return 0

        lax.fori_loop(0, tokens // 128, turn, 0)

    g = dot(wg_ref[...], aT_ref[...], TN)
    g_ref[...] = g
    u = dot(wu_ref[...], aT_ref[...], TN)
    u_ref[...] = u
    act_ref[...] = (g * sigmoid(g) * u).astype(BF)


def first(layer, x, w_gate, w_up):
    tokens, d = x.shape
    ff = w_gate.shape[-1]
    wspec = pl.BlockSpec((None, d, STEP), lambda j: (layer, 0, j))
    hidden = pl.BlockSpec((STEP, tokens), lambda j: (j, 0))
    return pl.pallas_call(
        first_kernel,
        name="first",
        grid=(ff // STEP,),
        in_specs=[whole((tokens, d)), wspec, wspec],
        out_specs=[whole((d, tokens)), whole((d, tokens)), hidden, hidden, hidden],
        out_shape=[
            jax.ShapeDtypeStruct((d, tokens), BF),
            jax.ShapeDtypeStruct((d, tokens), BF),
            jax.ShapeDtypeStruct((ff, tokens), F32),
            jax.ShapeDtypeStruct((ff, tokens), F32),
            jax.ShapeDtypeStruct((ff, tokens), BF),
        ],
        compiler_params=params(),
    )(x, w_gate, w_up)


def down_kernel(wd_ref, act_ref, xT_ref, dy_ref, hT_ref, aT_ref, dyT_ref):
    dyT_ref[...] = dy_ref[...].astype(F32).T.astype(BF)
    out = dot(wd_ref[...], act_ref[...], TN).astype(BF)
    h = xT_ref[...] + out
    hT_ref[...] = h
    aT_ref[...] = norm_rows(h.astype(F32)).astype(BF)


def down(layer, w_down, act, xT, dy):
    d, tokens = xT.shape
    ff = act.shape[0]
    column = pl.BlockSpec((d, TOK), lambda i: (0, i))
    return pl.pallas_call(
        down_kernel,
        name="down",
        grid=(tokens // TOK,),
        in_specs=[
            pl.BlockSpec((None, ff, d), lambda i: (layer, 0, 0), pipeline_mode=pl.Buffered(1)),
            pl.BlockSpec((ff, TOK), lambda i: (0, i)),
            column,
            pl.BlockSpec((TOK, d), lambda i: (i, 0)),
        ],
        out_specs=[column] * 3,
        out_shape=[jax.ShapeDtypeStruct((d, tokens), BF)] * 3,
        compiler_params=params(),
    )(w_down, act, xT, dy)


def hidden_back(g, u, da):
    da = da.astype(F32)
    s = sigmoid(g)
    silu = g * s
    return (da * u * (s + silu * (1.0 - s))).astype(BF), (da * silu).astype(BF)


def last_kernel(dyT_ref, aT_ref, wg_ref, wu_ref, wd_ref, act_ref, dgu_ref):
    g = dot(wg_ref[...], aT_ref[...], TN)
    u = dot(wu_ref[...], aT_ref[...], TN)
    da = dot(wd_ref[...], dyT_ref[...], NN).astype(BF)
    act_ref[...] = (g * sigmoid(g) * u).astype(BF)
    dgu_ref[0], dgu_ref[1] = hidden_back(g, u, da)


def last(layer, dyT, aT, w_gate, w_up, w_down):
    d, tokens = aT.shape
    ff = w_gate.shape[-1]
    wspec = pl.BlockSpec((None, d, STEP), lambda j: (layer, 0, j))
    return pl.pallas_call(
        last_kernel,
        name="last",
        grid=(ff // STEP,),
        in_specs=[whole((d, tokens)), whole((d, tokens)), wspec, wspec, pl.BlockSpec((None, STEP, d), lambda j: (layer, j, 0))],
        out_specs=[
            pl.BlockSpec((STEP, tokens), lambda j: (j, 0)),
            pl.BlockSpec((None, 2, STEP, tokens), lambda j: (j, 0, 0, 0)),
        ],
        out_shape=[
            jax.ShapeDtypeStruct((ff, tokens), BF),
            jax.ShapeDtypeStruct((ff // STEP, 2, STEP, tokens), BF),
        ],
        compiler_params=params(),
    )(dyT, aT, w_gate, w_up, w_down)


OFF_A, OFF_B, OFF_C, OFF_D, OFF_F = 0, 1, 3, 5, 7
N_G, N_R0, N_SB, N_RB, N_SC, N_RC, N_SD, N_RD, N_SO = 8, 6, 2, 6, 2, 4, 2, 4, 2
WIDE = STEP
MESH = pl.DeviceIdType.MESH


class Place:
    def __init__(self):
        me = lax.axis_index("dp")
        self.core = me % 2
        self.y = (me // 2) % SIDE
        self.x = me // (2 * SIDE)

    def number(self, x, y, core):
        return ((x % SIDE) * SIDE + y % SIDE) * 2 + core

    def other_core(self):
        return self.number(self.x, self.y, 1 - self.core)

    def first(self, odd):
        return self.x + odd * (self.y - self.x), self.y + odd * (self.x - self.y)

    def along_first(self, odd, by):
        return self.number(self.x + (1 - odd) * by, self.y + odd * by, self.core)

    def along_second(self, odd, by):
        return self.number(self.x + odd * by, self.y + (1 - odd) * by, self.core)

    def meet(self):
        barrier = pltpu.get_barrier_semaphore()
        others = [self.other_core()] + [f(0, by) for by in (1, 2, 3) for f in (self.along_first, self.along_second)]
        for other in others:
            pl.semaphore_signal(barrier, inc=1, device_id={"dp": other}, device_id_type=MESH)
        pl.semaphore_wait(barrier, len(others))


class Reducer:
    @staticmethod
    def scratch(r, w):
        dma = pltpu.SemaphoreType.DMA
        return [
            pltpu.VMEM((N_G, SIDE, SIDE, 2, r, w), BF),
            pltpu.VMEM((N_R0, SIDE, SIDE, r, w), BF),
            pltpu.VMEM((N_SB, 2, 4, r, w), BF),
            pltpu.VMEM((N_RB, 2, 4, r, w), BF),
            pltpu.VMEM((N_SC, 2, 2, r, w), BF),
            pltpu.VMEM((N_RC, 2, 2, r, w), BF),
            pltpu.VMEM((N_SD, 3, r, w), BF),
            pltpu.VMEM((N_RD, 3, r, w), BF),
            pltpu.VMEM((N_SO, r, w), F32),
            dma((N_G,)),
            dma((N_R0,)),
            dma((N_R0,)),
            dma((N_SB, 2)),
            dma((N_RB, 2)),
            dma((N_SC, 2)),
            dma((N_RC, 2)),
            dma((N_SD, 3)),
            dma((N_RD, 3)),
        ]

    def __init__(self, place, refs, finish):
        self.place, self.finish = place, finish
        (self.G, self.R0, self.SB, self.RB, self.SC, self.RC, self.SD, self.RD, self.SO) = refs[:9]
        (self.l_sem, self.a_send, self.a_recv, self.b_send, self.b_recv, self.c_send, self.c_recv, self.d_send, self.d_recv) = refs[9:]

    def remote(self, src, dst, send, recv, to):
        return pltpu.make_async_remote_copy(src_ref=src, dst_ref=dst, send_sem=send, recv_sem=recv, device_id={"dp": to}, device_id_type=MESH)

    def copy_a(self, k):
        s = k % N_R0
        return self.remote(self.G.at[k % N_G, :, :, 1 - self.place.core], self.R0.at[s], self.a_send.at[s], self.a_recv.at[s], self.place.other_core())

    def copy_b(self, k, way):
        s, r = k % N_SB, k % N_RB
        to = self.place.along_first(k % 2, 1 if way == 0 else SIDE - 1)
        return self.remote(self.SB.at[s, way], self.RB.at[r, way], self.b_send.at[s, way], self.b_recv.at[r, way], to)

    def copy_c(self, k, way):
        s, r = k % N_SC, k % N_RC
        to = self.place.along_first(k % 2, 1 if way == 0 else SIDE - 1)
        return self.remote(self.SC.at[s, way], self.RC.at[r, way], self.c_send.at[s, way], self.c_recv.at[r, way], to)

    def copy_d(self, k, by):
        s, r = k % N_SD, k % N_RD
        to = self.place.along_second(k % 2, by)
        return self.remote(self.SD.at[s, by - 1], self.RD.at[r, by - 1], self.d_send.at[s, by - 1], self.d_recv.at[r, by - 1], to)

    def pair(self, k, target, j):
        odd = k % 2
        x = target + odd * (j - target)
        y = j + odd * (target - j)
        return self.G[k % N_G, x, y, self.place.core].astype(F32) + self.R0[k % N_R0, x, y].astype(F32)

    def stage_a(self, k):
        self.copy_a(k).start()

    def stage_b(self, k):
        a = self.copy_a(k)
        a.wait_recv()
        a.wait_send()
        first, _ = self.place.first(k % 2)
        s = k % N_SB
        for way in range(2):
            for j in range(4):
                far = (j < 2) == (way == 0)
                target = (first + (2 if far else 1 if way == 0 else SIDE - 1)) % SIDE
                self.SB[s, way, j] = self.pair(k, target, j).astype(BF)
            self.copy_b(k, way).start()

    def stage_c(self, k):
        first, _ = self.place.first(k % 2)
        s, r = k % N_SC, k % N_RB
        for way in range(2):
            b = self.copy_b(k, way)
            b.wait_send()
            b.wait_recv()
            target = (first + (1 if way == 0 else SIDE - 1)) % SIDE
            for i in range(2):
                j = i + 2 * way
                self.SC[s, way, i] = (self.pair(k, target, j) + self.RB[r, way, j].astype(F32)).astype(BF)
            self.copy_c(k, way).start()

    def stage_d(self, k):
        for way in range(2):
            c = self.copy_c(k, way)
            c.wait_send()
            c.wait_recv()
        first, second = self.place.first(k % 2)
        b, c = k % N_RB, k % N_RC
        for by in (1, 2, 3, 0):
            j = (second + by) % SIDE
            high = j // 2
            total = self.pair(k, first, j) + self.RC[c, high, j % 2].astype(F32) + self.RB[b, 1 - high, j].astype(F32)
            if by:
                self.SD[k % N_SD, by - 1] = total.astype(BF)
                self.copy_d(k, by).start()
            else:
                self.SO[k % N_SO] = total

    def stage_f(self, k):
        total = self.SO[k % N_SO]
        for by in (1, 2, 3):
            d = self.copy_d(k, by)
            d.wait_send()
            d.wait_recv()
            total = total + self.RD[k % N_RD, by - 1].astype(F32)
        self.finish(k, total.astype(BF))

    def tick(self, t, low, high, load=None):
        for off, stage in ((OFF_F, self.stage_f), (OFF_D, self.stage_d), (OFF_C, self.stage_c), (OFF_B, self.stage_b), (OFF_A, self.stage_a)):
            k = t - off
            if isinstance(k, int):
                if low <= k < high:
                    stage(k)
                continue

            @pl.when(jnp.logical_and(k >= low, k < high))
            def _():
                if off == OFF_A and load is not None:
                    load(k).wait()
                stage(k)


def weights_kernel(shape, *refs):
    d, ff, tokens, own_gu, own_dn, packs = shape
    (aT0, act0, g0, u0, wd, hT, aT1, act1, dgu1, dyT, wg, wu) = refs[:12]
    out_dn, out_gate, out_up, ssq_out, gdn = refs[12:17]
    res, stream, acc, wbuf, stage, ready, ssq, peer = refs[17:25]
    res_sem, stream_sem, acc_sem, w_sem, stage_sem, ready_sem, q_send, q_recv = refs[25:33]
    place = Place()
    tiles = ff // STEP
    half = d // 2
    assert half == STEP
    dn_tile = 4 * own_dn
    dn_tiles = ff // dn_tile
    layer_chunks = 3 * tiles
    assert packs == tiles and packs <= dn_tiles

    place.meet()
    ssq[...] = jnp.zeros_like(ssq)

    def put(k, kind=0):
        layer, i = 1 - k // layer_chunks, (k // 3) % tiles
        at = pl.ds(pl.multiple_of(i * STEP, 128), STEP)
        to = out_dn.at[layer, i] if kind == 0 else (out_gate, out_up)[kind - 1].at[layer, :, at]
        return pltpu.make_async_copy(ready.at[k % 2], to, ready_sem.at[k % 2])

    def finish(k, g):
        @pl.when(k >= 2)
        def _():
            put(k - 2).wait()

        ready[k % 2] = g
        for kind in range(3):

            @pl.when(k % 3 == kind)
            def _():
                put(k, kind).start()

        g = g.astype(F32)
        g = g * g
        rows = g[0:8]
        for i in range(8, g.shape[0], 8):
            rows = rows + g[i : i + 8]
        lanes = rows[:, 0:128]
        for i in range(128, g.shape[1], 128):
            lanes = lanes + rows[:, i : i + 128]
        ssq[0] = ssq[0] + lanes

    eng = Reducer(place, refs[33:], finish)

    def copy(src, dst, sem):
        return pltpu.make_async_copy(src, dst, sem)

    def rows(i, size):
        return pl.ds(pl.multiple_of(i * size, 16), size)

    def load_res(which, ref):
        return copy(ref, res.at[which], res_sem.at[which])

    def stream_gu(i, slot):
        return copy(dgu1.at[i], stream.at[slot], stream_sem.at[slot])

    def stream_dn(ref, i, slot):
        return copy(ref.at[rows(i, dn_tile), :], stream.at[slot, pl.ds(0, dn_tile)], stream_sem.at[slot])

    def w_tile(i, part):
        at = pl.ds(pl.multiple_of(i * STEP, 128), STEP)
        return [copy(w.at[1, pl.ds(part * half, half), at], wbuf.at[:, pl.ds(n * STEP, STEP)], w_sem.at[n]) for n, w in enumerate((wg, wu))]

    def hidden_tile(i):
        return [
            copy(g0.at[rows(i, STEP), :], acc.at[pl.ds(0, STEP)], acc_sem.at[0]),
            copy(u0.at[rows(i, STEP), :], acc.at[pl.ds(STEP, STEP)], acc_sem.at[1]),
            copy(wd.at[0, rows(i, STEP), :], wbuf, w_sem.at[0]),
        ]

    def wgrad(which, slot, part, first):
        product = dot(res[which, part * half : (part + 1) * half, :], stream[slot], NT)
        for c in range(2):
            for q in range(SIDE * SIDE):
                x, y, core = part * 2 + q // (2 * SIDE), (q // 2) % SIDE, q % 2
                eng.G[(first + c) % N_G, x, y, core] = product[q * own_gu : (q + 1) * own_gu, c * WIDE : (c + 1) * WIDE].astype(BF)

    stage[...] = jnp.zeros_like(stage)
    full = own_dn // own_gu
    rest = own_dn - full * own_gu
    blocks = d // WIDE

    def stage_out(number, i, s):
        return copy(stage.at[s], gdn.at[number, :, i // 2, pl.ds((i % 2) * 2, 2)], stage_sem.at[s])

    def load_dn(number, chunk, k):
        return copy(gdn.at[number, chunk], eng.G.at[k % N_G], eng.l_sem.at[k % N_G])

    def down_gradient(number, which, i, slot):
        s = i % 2

        @pl.when(i >= 2)
        def _():
            stage_out(number, i - 2, s).wait()

        product = dot(stream[slot, 0:dn_tile, :], res[which], NT)
        for q in range(4):
            for b in range(blocks):
                lanes = slice(b * WIDE, (b + 1) * WIDE)
                for p in range(full):
                    r = q * own_dn + p * own_gu
                    stage[s, p * blocks + b, q // 2, q % 2] = product[r : r + own_gu, lanes].astype(BF)
                r = q * own_dn + full * own_gu
                stage[s, full * blocks + b // 2, q // 2, q % 2, (b % 2) * rest : (b % 2 + 1) * rest] = product[r : r + rest, lanes].astype(BF)
        stage_out(number, i, s).start()

    load_res(1, dyT).start()
    stream_dn(act1, 0, 0).start()
    load_res(0, aT1).start()
    for one in w_tile(0, 0):
        one.start()
    acc[...] = jnp.zeros_like(acc)
    load_res(1, dyT).wait()

    def down1(i, _):
        slot = i % 2
        stream_dn(act1, i, slot).wait()

        @pl.when(i + 1 < dn_tiles)
        def _():
            stream_dn(act1, i + 1, 1 - slot).start()

        @pl.when(i + 1 == dn_tiles)
        def _():
            stream_gu(0, 1 - slot).start()

        down_gradient(0, 1, i, slot)
        return 0

    lax.fori_loop(0, dn_tiles, down1, 0)
    for i in range(dn_tiles - 2, dn_tiles):
        stage_out(0, i, i % 2).wait()
    load_dn(0, 0, 0).start()
    load_res(0, aT1).wait()

    def layer1(i, _):
        slot = (dn_tiles + i) % 2
        load = lambda k: load_dn(0, k // 3, k)
        stream_gu(i, slot).wait()

        @pl.when(i + 1 < tiles)
        def _():
            stream_gu(i + 1, 1 - slot).start()

        @pl.when(i + 1 == tiles)
        def _():
            copy(hT, stream.at[1 - slot], stream_sem.at[1 - slot]).start()

        wgrad(0, slot, 0, 3 * i + 1)
        eng.tick(3 * i, 0, layer_chunks, load)

        @pl.when(i + 1 < tiles)
        def _():
            load(3 * i + 3).start()

        for part in range(2):
            if part:
                wgrad(0, slot, 1, 3 * i + 1)
                eng.tick(3 * i + 1, 0, layer_chunks)
            for one in w_tile(i, part):
                one.wait()
            acc[part * half : (part + 1) * half] += dot(wbuf[...], stream[slot], NN)
            if not part:
                for one in w_tile(i, 1):
                    one.start()

        @pl.when(i + 1 < tiles)
        def _():
            for one in w_tile(i + 1, 0):
                one.start()

        eng.tick(3 * i + 2, 0, layer_chunks)
        return 0

    lax.fori_loop(0, tiles, layer1, 0)

    s_h = (dn_tiles + tiles) % 2
    stream_dn(act0, 0, 1 - s_h).start()
    copy(hT, stream.at[s_h], stream_sem.at[s_h]).wait()

    def back_norm(i, _):
        at = pl.ds(pl.multiple_of(i * 128, 128), 128)
        h = stream[s_h, :, at].astype(F32)
        da = acc[:, at].astype(BF).astype(F32)
        scale = lax.rsqrt(jnp.mean(h * h, 0, keepdims=True) + 1e-6)
        along = jnp.mean(da * h, 0, keepdims=True)
        dh = da * scale - h * (scale * scale * scale * along)
        res[0, :, at] = res[1, :, at] + dh.astype(BF)
        return 0

    lax.fori_loop(0, tokens // 128, back_norm, 0)
    for one in hidden_tile(0):
        one.start()
    load_res(1, aT0).start()

    def down0(i, _):
        slot = (1 - s_h + i) % 2
        stream_dn(act0, i, slot).wait()

        @pl.when(i + 1 < dn_tiles)
        def _():
            stream_dn(act0, i + 1, 1 - slot).start()

        eng.tick(layer_chunks + i, 0, layer_chunks)
        down_gradient(1, 0, i, slot)
        return 0

    assert dn_tiles >= OFF_F
    lax.fori_loop(0, dn_tiles, down0, 0)
    for i in range(dn_tiles - 2, dn_tiles):
        stage_out(1, i, i % 2).wait()
    load_dn(1, 0, layer_chunks).start()
    load_res(1, aT0).wait()

    def layer0(i, _):
        base = layer_chunks + 3 * i
        load = lambda k: load_dn(1, k // 3 - tiles, k)

        @pl.when(i > 0)
        def _():
            eng.tick(base - 2, layer_chunks, 2 * layer_chunks)

        for one in hidden_tile(i):
            one.wait()
        for part in range(2):
            at = pl.ds(part * (tokens // 2), tokens // 2)
            da = dot(wbuf[...], res[0, :, at], NN).astype(BF)
            stream[0, 0:STEP, at], stream[0, STEP:, at] = hidden_back(acc[0:STEP, at], acc[STEP:, at], da)

        @pl.when(i > 0)
        def _():
            eng.tick(base - 1, layer_chunks, 2 * layer_chunks)
            load(base).start()

        @pl.when(i + 1 < tiles)
        def _():
            for one in hidden_tile(i + 1):
                one.start()

        wgrad(1, 0, 0, base + 1)
        eng.tick(base, layer_chunks, 2 * layer_chunks, load)
        wgrad(1, 0, 1, base + 1)
        return 0

    lax.fori_loop(0, tiles, layer0, 0)

    def drain(i, _):
        eng.tick(2 * layer_chunks - 2 + i, layer_chunks, 2 * layer_chunks)
        return 0

    lax.fori_loop(0, 2 + OFF_F, drain, 0)
    for k in range(2 * layer_chunks - 2, 2 * layer_chunks):
        put(k).wait()

    for number, peers in enumerate(([place.other_core()], [place.along_first(0, by) for by in (1, 2, 3)], [place.along_second(0, by) for by in (1, 2, 3)])):
        at = (0, 1, 4)[number]
        copies = []
        for i, to in enumerate(peers):
            copies.append(eng.remote(ssq.at[number], peer.at[at + i], q_send.at[at + i], q_recv.at[at + i], to))
            copies[-1].start()
        total = ssq[number]
        for i, one in enumerate(copies):
            one.wait_recv()
            total = total + peer[at + i]
        for one in copies:
            one.wait_send()
        if number < 2:
            ssq[number + 1] = total
        else:
            ssq_out[...] = total


def weight_gradients(aT0, act0, g0, u0, wd, hT, aT1, act1, dgu1, dyT, wg, wu, n):
    d, tokens = aT0.shape
    ff = act0.shape[0]
    tiles = ff // STEP
    own_gu, own_dn = d // n, ff // n
    blocks = d // WIDE
    full = own_dn // own_gu
    rest = own_dn - full * own_gu
    assert 2 * rest <= own_gu
    packs = full * blocks + -(-blocks // 2)
    dma = pltpu.SemaphoreType.DMA
    flat = (aT0, act0, g0, u0, wd, hT, aT1, act1, dgu1.reshape(tiles, 2 * STEP, tokens), dyT, wg, wu)
    vm = pl.BlockSpec(memory_space=pltpu.VMEM)
    hbm = pl.BlockSpec(memory_space=pl.ANY)
    dn, gate, up, squares, _ = pl.pallas_call(
        lambda *refs: weights_kernel((d, ff, tokens, own_gu, own_dn, packs), *refs),
        name="weights",
        in_specs=[hbm] * len(flat),
        out_specs=[hbm, hbm, hbm, vm, hbm],
        out_shape=[
            jax.ShapeDtypeStruct((2, packs, own_gu, WIDE), BF),
            jax.ShapeDtypeStruct((2, own_gu, ff), BF),
            jax.ShapeDtypeStruct((2, own_gu, ff), BF),
            jax.ShapeDtypeStruct((8, 128), F32),
            jax.ShapeDtypeStruct((2, packs, SIDE, SIDE, 2, own_gu, WIDE), BF),
        ],
        scratch_shapes=[
            pltpu.VMEM((2, d, tokens), BF),
            pltpu.VMEM((2, 2 * STEP, tokens), BF),
            pltpu.VMEM((d, tokens), F32),
            pltpu.VMEM((STEP, d), BF),
            pltpu.VMEM((2, packs, 2, 2, own_gu, WIDE), BF),
            pltpu.VMEM((2, own_gu, WIDE), BF),
            pltpu.VMEM((3, 8, 128), F32),
            pltpu.VMEM((7, 8, 128), F32),
            dma((2,)),
            dma((2,)),
            dma((2,)),
            dma((2,)),
            dma((2,)),
            dma((2,)),
            dma((7,)),
            dma((7,)),
        ]
        + Reducer.scratch(own_gu, WIDE),
        compiler_params=params(collective_id=1, has_side_effects=True),
        cost_estimate=pl.CostEstimate(flops=18 * d * ff * tokens, bytes_accessed=2**27, transcendentals=0),
    )(*flat)
    top = dn[:, : full * blocks].reshape(2, full, blocks, own_gu, WIDE).transpose(0, 1, 3, 2, 4).reshape(2, full * own_gu, d)
    low = dn[:, full * blocks :, : 2 * rest].reshape(2, -1, rest, WIDE)[:, :blocks].transpose(0, 2, 1, 3).reshape(2, rest, d)
    return (gate, up, jnp.concatenate([top, low], 1)), jnp.sum(squares)


def gather_kernel(own_ref, out_ref, land, own_sem, out_sem, send, recv):
    place = Place()
    me = place.number(place.x, place.y, place.core)
    mine = pltpu.make_async_copy(own_ref, land.at[:, me], own_sem)
    mine.start()
    place.meet()
    mine.wait()
    started = []

    def at(half, first, second, core=None):
        x, y = (first, second) if half == 0 else (second, first)
        return place.number(place.x + x, place.y + y, place.core if core is None else core)

    def copy(half, number, slot, to):
        strip = land.at[half, number]
        return pltpu.make_async_remote_copy(
            src_ref=strip, dst_ref=strip, send_sem=send.at[half, slot], recv_sem=recv.at[half, slot], device_id={"dp": to}, device_id_type=MESH
        )

    def go(*what):
        started.append(copy(*what))
        started[-1].start()

    def from_side(first, way):
        return 3 + 2 * first + way

    def from_far(first):
        return 11 + first

    def from_core(first, second):
        return 15 + 4 * first + second

    sides = (1, 3)
    for half in range(2):
        for by in (1, 3, 2):
            go(half, me, by - 1, at(half, by, 0))
    for half in range(2):
        for way in range(2):
            go(half, me, from_side(0, way), at(half, 0, sides[way]))
    for half in range(2):
        go(half, me, from_core(0, 0), place.other_core())
    for by in (1, 3, 2):
        for half in range(2):
            first = SIDE - by
            owner = at(half, first, 0)
            copy(half, owner, by - 1, me).wait_recv()
            for way in range(2):
                go(half, owner, from_side(first, way), at(half, 0, sides[way]))
            go(half, owner, from_core(first, 0), place.other_core())
    for first in (0, 3, 1, 2):
        for half in range(2):
            for way in range(2):
                second = SIDE - sides[way]
                owner = at(half, first, second)
                copy(half, owner, from_side(first, way), me).wait_recv()
                if (first < 2) == (way == 0):
                    go(half, owner, from_far(first), at(half, 0, sides[way]))
                go(half, owner, from_core(first, second), place.other_core())
    for first in (0, 3, 1, 2):
        for half in range(2):
            owner = at(half, first, 2)
            copy(half, owner, from_far(first), me).wait_recv()
            go(half, owner, from_core(first, 2), place.other_core())
    for first in range(SIDE):
        for second in range(SIDE):
            for half in range(2):
                copy(half, at(half, first, second, 1 - place.core), from_core(first, second), me).wait_recv()
    outs = []
    each = land.shape[1] // 8
    for i in range(8):
        part = pl.ds(i * each, each)
        outs.append(pltpu.make_async_copy(land.at[:, part], out_ref.at[:, part], out_sem.at[i]))
        outs[-1].start()
    for one in started:
        one.wait_send()
    for one in outs:
        one.wait()


def gather(own, n):
    layers, rows, columns = own.shape
    assert layers == 2
    dma = pltpu.SemaphoreType.DMA
    slots = 15 + SIDE * SIDE
    size = 2 * own.size * n
    out = pl.pallas_call(
        gather_kernel,
        name="gather",
        in_specs=[pl.BlockSpec(memory_space=pl.ANY)],
        out_specs=pl.BlockSpec(memory_space=pl.ANY),
        out_shape=jax.ShapeDtypeStruct((layers, n, rows, columns), BF),
        scratch_shapes=[pltpu.VMEM((layers, n, rows, columns), BF), dma, dma((8,)), dma((2, slots)), dma((2, slots))],
        compiler_params=pltpu.CompilerParams(vmem_limit_bytes=size + 2**21, collective_id=2, has_side_effects=True),
        cost_estimate=pl.CostEstimate(flops=10**11, bytes_accessed=size, transcendentals=0),
    )(own)
    return out.reshape(layers, n * rows, columns)


def settle_kernel(in_ref, out_ref):
    out_ref[...] = in_ref[...]


def settle(w):
    layers, rows, columns = w.shape
    block = pl.BlockSpec((None, 320, columns), lambda i, j: (i, j, 0))
    return pl.pallas_call(
        settle_kernel,
        name="settle",
        grid=(layers, rows // 320),
        in_specs=[block],
        out_specs=block,
        out_shape=jax.ShapeDtypeStruct(w.shape, BF),
        compiler_params=pltpu.CompilerParams(vmem_limit_bytes=2**24),
        cost_estimate=pl.CostEstimate(flops=10**10, bytes_accessed=4 * w.size, transcendentals=0),
    )(w)


def join_kernel(in_ref, out_ref, wide):
    strips, rows, _ = in_ref.shape
    for i in range(strips):
        wide[i * rows : (i + 1) * rows, :] = in_ref[i].astype(F32)
    out_ref[...] = wide[...].astype(BF)


def join(parts):
    n, layers, rows, columns = parts.shape
    size = 4 * rows
    return pl.pallas_call(
        join_kernel,
        name="join",
        grid=(layers, n // 4),
        in_specs=[pl.BlockSpec((4, None, rows, columns), lambda i, j: (j, i, 0, 0))],
        out_specs=pl.BlockSpec((None, size, columns), lambda i, j: (i, j, 0)),
        out_shape=jax.ShapeDtypeStruct((layers, n * rows, columns), BF),
        scratch_shapes=[pltpu.VMEM((size, columns), F32)],
        compiler_params=pltpu.CompilerParams(vmem_limit_bytes=2**24),
        cost_estimate=pl.CostEstimate(flops=10**10, bytes_accessed=4 * parts.size, transcendentals=0),
    )(parts)


def adamw(w, m, v, g):
    m = 0.9 * m + 0.1 * g
    v = 0.95 * v + 0.05 * g * g
    step = m * lax.rsqrt(v + 1e-8) + 0.1 * w
    return (w - 0.02 * step).astype(BF), m, v


def solution(mesh):
    n = mesh.shape["dp"]
    assert n == 2 * SIDE * SIDE and math.isqrt(n // 2) == SIDE

    def one(x, dy, wg, wu, wd, *moments):
        x, dy = x[0], dy[0]
        xT, aT0, g0, u0, act0 = first(0, x, wg, wu)
        hT, aT1, dyT = down(0, wd, act0, xT, dy)
        act1, dgu1 = last(1, dyT, aT1, wg, wu, wd)
        gradients, squares = weight_gradients(aT0, act0, g0, u0, wd, hT, aT1, act1, dgu1, dyT, wg, wu, n)
        count = wg.size + wu.size + wd.size
        factor = jnp.minimum(1.0, 0.5 * lax.rsqrt(squares / count + 1e-30))
        me = lax.axis_index("dp")
        ws, ms, vs = [], [], []
        for w, m, v, g in zip((wg, wu, wd), moments[:3], moments[3:], gradients, strict=True):
            mine = lax.dynamic_slice_in_dim(w, me * m.shape[1], m.shape[1], 1)
            w, m, v = adamw(mine.astype(F32), m, v, g.astype(F32) * factor)
            ws.append(w)
            ms.append(m)
            vs.append(v)
        new_down = join(lax.all_gather(ws[2], "dp", axis=0))
        new_gate, ms[2], vs[2] = lax.optimization_barrier((gather(ws[0], n), ms[2], vs[2]))
        new_gate = settle(new_gate)
        new_up = settle(lax.all_gather(ws[1], "dp", axis=1, tiled=True))
        return (new_gate, new_up, new_down, *ms, *vs)

    seq = P(("rep", "dp"))
    own = P(None, "dp")
    return jax.shard_map(
        one,
        mesh=mesh,
        in_specs=(seq, seq, P(), P(), P()) + (own,) * 6,
        out_specs=(P("rep"),) * 3 + (P("rep", "dp"),) * 6,
        check_vma=False,
    )
```
